32 devices in a mesh: grp: 1, exp: 32 (over z, y, x, core).
Axes of the slice: x: 2, y: 2, z: 4, core: 2. Of those that a mesh axis runs over, the one named last changes fastest.
Arguments:
- tokens: bfloat16 [512, 2048], P(('grp', 'exp')), may hold values from -6 to 6
- routed_expert_index: int32 [512, 6], P(('grp', 'exp')), may hold values from 0 to 15, all different within a row; in each aligned block of 16 rows (0 to 15, 16 to 31, ...) at most 8 rows name the same one
- routing_gate_weight: float32 [512, 6], P(('grp', 'exp')), may hold values from 0.05 to 0.5
- token_adapter_index: int32 [512], P('grp'), may hold values from 0 to 511
- gate_weight_pieces: bfloat16 [32, 2048, 704], P('exp'), may hold values from -0.125 to 0.125
- up_weight: bfloat16 [32, 2048, 704], P('exp'), may hold values from -0.125 to 0.125
- down_weight: bfloat16 [32, 704, 2048], P('exp'), may hold values from -0.15625 to 0.15625
- adapter_down_matrix: bfloat16 [2048, 8192], P('exp'), may hold values from -0.125 to 0.125
- adapter_up_matrix: bfloat16 [2048, 8192], P('exp'), may hold values from -1.5 to 1.5
Outputs:
- mixed: bfloat16 [512, 2048], P(('grp', 'exp'))
The draws below stay inside these ranges and needn't reach their ends.
Inputs may be any that keep to these rules, and one draw needn't show every extreme that they name: `routed_expert_index`: each token names 6 different experts; among the 16 tokens of one index of exp (aligned blocks of rows) no expert is named more than 8 times.
All inputs are finite; a program needn't handle non-finite values.
Results may differ from the reference program's by a relative error of at most 0.009.
Values may be sent and summed in bfloat16 or wider, within the bound.
No kernel may reach another device: no remote copies, remote signals or barrier semaphores. Data moves between devices by JAX's collectives and lax.ppermute only.
A program may use at most 128 MiB of HBM per device.

```python
import math
import jax
import jax.numpy as jnp
import numpy as np
from jax import lax

MODEL_DIM = 2048
FF = 1408
TOP = 6
ADAPTER_RANK = 16
ADAPTER_COUNT = 512
TOKENS_PER_SHARD = 16
EXPERTS = 16
TOKENS = 512
CAP = 8
N_EXP = 32


def plant(entries, key, smallest, largest):
    index_at = [jax.random.randint(jax.random.fold_in(key, axis), (), 0, length) for axis, length in enumerate(entries.shape)]
    main_axis = entries.shape.index(max(entries.shape))
    next_to = index_at[:main_axis] + [(index_at[main_axis] + 1) % entries.shape[main_axis]] + index_at[main_axis + 1:]
    return entries.at[tuple(index_at)].set(smallest).at[tuple(next_to)].set(largest)


def block_levels(own_key, dims, cuts, least, largest):
    def one(axis_at, parts):
        heights = jax.random.uniform(jax.random.fold_in(jax.random.fold_in(own_key, 6), axis_at), (parts,), jnp.float32, least / len(cuts), largest / len(cuts))
        return jnp.repeat(jnp.exp(heights), dims[axis_at] // parts).reshape((-1,) + (1,) * (len(dims) - axis_at - 1))

    factor_of = one(*cuts[0])
    for cut in cuts[1:]:
        factor_of = factor_of * one(*cut)
    return factor_of


def rank_bounds(number_of, slope):
    weights = [(1 << 20) // math.isqrt(grade ** slope) + 1 for grade in range(1, number_of + 1)]
    scale = 1 + sum(weights) // (1 << 30)
    return np.cumsum(np.array([max(1, weight // scale) for weight in weights]))


def skewed_ids(stream_key, extent, number_of, lean):
    listing = rank_bounds(number_of, lean)
    ticket = jax.random.randint(jax.random.fold_in(stream_key, 1), extent, 0, int(listing[number_of - 1]))
    standing = jnp.searchsorted(jnp.asarray(listing, jnp.int32), ticket, side="right")
    return jax.random.permutation(jax.random.fold_in(stream_key, 2), number_of)[standing].astype(jnp.int32)


def assign_block(rng, own, number, rows, number_of, top, most, skew):
    order = jax.random.permutation(rng, number_of)
    heavy_load, ordinary = shares(number_of, rows * top, most, skew, True), shares(number_of, rows * top, most, skew, False)
    places = jnp.arange(number_of)

    def named(tallies, turn):
        used = int((tallies > 0).sum())
        fixed = max(1, used // 4)
        passed = fixed + (places - fixed + turn * (used - fixed)) % max(1, number_of - fixed)
        return jnp.zeros((number_of,), jnp.int32).at[order[jnp.where(places < fixed, places, passed)]].set(jnp.asarray(tallies, jnp.int32))

    tallies = jnp.where(number % 4 == 0, named(heavy_load, number // 4), named(ordinary, number - number // 4 - 1))
    mixed = jax.random.permutation(jax.random.fold_in(own, 3), number_of)
    donor, sink = mixed[0:number_of // 2 * 2:2], mixed[1:number_of // 2 * 2:2]
    room = jnp.minimum(tallies[donor] - 1, most - tallies[sink]) // 2
    room = jnp.where((donor == order[0]) | (sink == order[0]) | (tallies[sink] == 0), 0, jnp.maximum(room, 0))
    passed = jax.random.randint(jax.random.fold_in(own, 4), (number_of // 2,), 0, 1 << 20) % (room + 1)
    tallies = tallies.at[donor].add(-passed).at[sink].add(passed)
    members = jnp.searchsorted(jnp.cumsum(tallies), jnp.arange(rows * top), side="right").astype(jnp.int32)
    table = members.reshape(top, rows).T
    table = table[jax.random.permutation(jax.random.fold_in(own, 1), rows)]
    turn = jax.random.randint(jax.random.fold_in(own, 2), (rows, 1), 0, top)
    return jnp.take_along_axis(table, (jnp.arange(top)[None, :] + turn) % top, axis=1)


def shares(count, total, limit, skew, full):
    loads = [(1 << 20) // math.isqrt(rank ** skew) + 1 for rank in range(1, count + 1)]
    largest = limit if full else min(limit, max(-(-total // count), total * loads[0] // sum(loads)))
    least = 1 if total - largest >= count - 1 else 0
    counts, rest = [largest] + [least] * (count - 1), total - largest - least * (count - 1)
    while rest > 0:
        free = [i for i in range(1, count) if counts[i] < largest] or [i for i in range(1, count) if counts[i] < limit]
        whole, left = sum([loads[i] for i in free]), rest
        for i in free:
            more = min(limit - counts[i], max(1, left * loads[i] // whole), rest)
            counts[i] = counts[i] + more
            rest = rest - more
    return np.array(counts)


def gaussian(stream_key, extent, width, limit, shards=(), kind=jnp.bfloat16):
    drawn = jax.random.normal(stream_key, extent, jnp.float32) * width
    if len(shards) > 0:
        drawn = block_levels(stream_key, extent, shards, -0.22, 0.18) * drawn
    return jnp.clip(drawn, min=-limit, max=limit).astype(kind)


def setup_inputs(seed: int = 0, part: int = 0) -> dict:
    splits = jax.random.split(jax.random.key(seed), 10)
    part_keys = jax.random.split(jax.random.fold_in(splits[9], part), 10)
    tokens = gaussian(part_keys[0], (TOKENS, MODEL_DIM), 1.0, 6.0, ((0, 32),))
    routed_expert_index_keys = jax.random.split(jax.random.fold_in(part_keys[1], 1), TOKENS // TOKENS_PER_SHARD)
    routed_expert_index_turns = jax.random.permutation(jax.random.fold_in(part_keys[1], 3), TOKENS // TOKENS_PER_SHARD)
    routed_expert_index = jax.vmap(lambda own, number: assign_block(jax.random.fold_in(part_keys[1], 2), own, number, TOKENS_PER_SHARD, EXPERTS, TOP, CAP, 2))(routed_expert_index_keys, routed_expert_index_turns).reshape((TOKENS, TOP))
    routing_gate_weight = jnp.clip(jnp.exp(math.log(0.5) - 2.3025851 * jax.random.uniform(part_keys[2], (TOKENS, TOP), jnp.float32) ** block_levels(part_keys[2], (TOKENS, TOP), ((0, 32),), -0.2, 0.2)), 0.05, 0.5)
    token_adapter_index = plant(skewed_ids(part_keys[3], (TOKENS,), ADAPTER_COUNT, 2), jax.random.fold_in(part_keys[3], 3), 0, ADAPTER_COUNT - 1).astype(jnp.int32)
    gate_weight_pieces = gaussian(splits[4], (2 * EXPERTS, MODEL_DIM, FF // 2), MODEL_DIM ** -0.5, 0.125, ((0, 32),))
    up_weight = gaussian(splits[5], (2 * EXPERTS, MODEL_DIM, FF // 2), MODEL_DIM ** -0.5, 0.125, ((0, 32),))
    down_weight = gaussian(splits[6], (2 * EXPERTS, FF // 2, MODEL_DIM), FF ** -0.5, 0.15625, ((0, 32),))
    adapter_down_matrix = gaussian(splits[7], (MODEL_DIM, ADAPTER_COUNT * ADAPTER_RANK), MODEL_DIM ** -0.5, 0.125, ((0, 32),))
    adapter_up_matrix = gaussian(splits[8], (MODEL_DIM, ADAPTER_COUNT * ADAPTER_RANK), ADAPTER_RANK ** -0.5, 1.5, ((0, 32),))
    return dict(tokens=tokens, routed_expert_index=routed_expert_index, routing_gate_weight=routing_gate_weight, token_adapter_index=token_adapter_index, gate_weight_pieces=gate_weight_pieces, up_weight=up_weight, down_weight=down_weight, adapter_down_matrix=adapter_down_matrix, adapter_up_matrix=adapter_up_matrix)


def reference(tokens, routed_expert_index, routing_gate_weight, token_adapter_index, gate_weight_pieces, up_weight, down_weight, adapter_down_matrix, adapter_up_matrix):
    flat_ids = routed_expert_index.reshape(N_EXP, TOKENS_PER_SHARD * TOP)
    one_hot = (flat_ids[:, :, None] == jnp.arange(EXPERTS, dtype=jnp.int32)[None, None, :]).astype(jnp.int32)
    counted = jnp.cumsum(one_hot, axis=1)
    position = jnp.sum(one_hot * counted, axis=2) - 1
    block_ids = jnp.arange(N_EXP, dtype=jnp.int32)[:, None]
    column = (block_ids * CAP + position).reshape(-1).astype(jnp.int32)
    expert_col = flat_ids.reshape(-1).astype(jnp.int32)
    token_col = (jnp.arange(TOKENS * TOP, dtype=jnp.int32) // TOP).astype(jnp.int32)
    row_table = jnp.full((EXPERTS, N_EXP * CAP), TOKENS, jnp.int32).at[expert_col, column].set(token_col)
    row_gates = jnp.zeros((EXPERTS, N_EXP * CAP), jnp.float32).at[expert_col, column].set(routing_gate_weight.reshape(-1))
    padded = jnp.concatenate([tokens, jnp.zeros((1, MODEL_DIM), tokens.dtype)], axis=0)

    def one_expert(summed, expert):
        rows_index = row_table[expert]
        row_block = padded[rows_index]
        output = jnp.zeros((row_block.shape[0], MODEL_DIM), jnp.float32)
        for which in range(2):
            slab_index = 2 * expert + which
            gate_act = jnp.dot(row_block, gate_weight_pieces[slab_index], preferred_element_type=jnp.float32)
            up_act = jnp.dot(row_block, up_weight[slab_index], preferred_element_type=jnp.float32)
            hidden = (jax.nn.silu(gate_act) * up_act).astype(jnp.bfloat16)
            output = output + jnp.dot(hidden, down_weight[slab_index], preferred_element_type=jnp.float32)
        summed = summed.at[rows_index].add(row_gates[expert][:, None] * output)
        return summed, None

    start = jnp.zeros((TOKENS + 1, MODEL_DIM), jnp.float32)
    routed, _ = lax.scan(one_expert, start, jnp.arange(EXPERTS, dtype=jnp.int32))
    routed = routed[:TOKENS]

    down_adapter_matrix = adapter_down_matrix.reshape(MODEL_DIM, ADAPTER_COUNT, ADAPTER_RANK)
    up_adapter_matrix = adapter_up_matrix.reshape(MODEL_DIM, ADAPTER_COUNT, ADAPTER_RANK)

    def adapter_block_rows(input_rows):
        x_block, id_block = input_rows
        down_selected = down_adapter_matrix[:, id_block, :].astype(jnp.float32)
        low_rank = jnp.einsum("td,dtr->tr", x_block.astype(jnp.float32), down_selected).astype(jnp.bfloat16)
        up_selected = up_adapter_matrix[:, id_block, :].astype(jnp.float32)
        return jnp.einsum("tr,dtr->td", low_rank.astype(jnp.float32), up_selected).astype(jnp.bfloat16)

    lowrank_delta = lax.map(adapter_block_rows, (tokens.reshape(N_EXP, TOKENS_PER_SHARD, MODEL_DIM), token_adapter_index.reshape(N_EXP, TOKENS_PER_SHARD)))
    lowrank_delta = lowrank_delta.reshape(TOKENS, MODEL_DIM)
    return (routed + lowrank_delta.astype(jnp.float32)).astype(jnp.bfloat16)
```

```python
import functools

import jax
import jax.numpy as jnp
from jax import lax
from jax.experimental import pallas as pl
from jax.experimental.pallas import tpu as pltpu
from jax.sharding import Mesh, PartitionSpec as P

TOP = 6
ADAPTER_RANK = 16
CORES = 2


def slot_tables(ids_t, gates_t, experts, capacity):
    tok = ids_t.shape[1]
    shape = (experts * capacity, tok)
    row = lax.broadcasted_iota(jnp.int32, shape, 0)
    expert = row // capacity
    chosen = jnp.zeros(shape, jnp.float32)
    weight = jnp.zeros(shape, jnp.float32)
    for k in range(TOP):
        hit = expert == ids_t[k : k + 1, :]
        chosen = chosen + jnp.where(hit, 1.0, 0.0)
        weight = weight + jnp.where(hit, gates_t[k : k + 1, :], 0.0)
    earlier = (
        lax.broadcasted_iota(jnp.int32, (tok, tok), 0) < lax.broadcasted_iota(jnp.int32, (tok, tok), 1)
    ).astype(jnp.float32)
    position = jnp.dot(
        chosen.astype(jnp.bfloat16), earlier.astype(jnp.bfloat16), preferred_element_type=jnp.float32
    )
    slot = (row - expert * capacity).astype(jnp.float32)
    placed = jnp.where(position == slot, chosen, 0.0)
    return placed, placed * weight


def pack_kernel(tokens, ids_t, gates_t, message, combine, *, experts, capacity, chip_features):
    width = tokens.shape[1]
    placed, weighted = slot_tables(ids_t[...], gates_t[...], experts, capacity)
    combine[...] = weighted
    message[:, :width] = jnp.dot(
        placed.astype(jnp.bfloat16), tokens[...], preferred_element_type=jnp.float32
    ).astype(jnp.bfloat16)
    for chip in range(experts):
        for part in range(tokens.shape[0] // capacity):
            message[
                chip * capacity : (chip + 1) * capacity,
                width + part * chip_features : width + (part + 1) * chip_features,
            ] = tokens[
                part * capacity : (part + 1) * capacity,
                chip * chip_features : (chip + 1) * chip_features,
            ]


def weighted_rows(combine, rows):
    high = combine.astype(jnp.bfloat16)
    low = (combine - high.astype(jnp.float32)).astype(jnp.bfloat16)
    dims = (((0,), (0,)), ((), ()))
    return lax.dot_general(high, rows, dims, preferred_element_type=jnp.float32) + lax.dot_general(
        low, rows, dims, preferred_element_type=jnp.float32
    )


def finish_kernel(message, combine, out, *, experts, capacity, chip_features):
    width = out.shape[1]
    routed = weighted_rows(combine[...], message[:, :width])
    for chip in range(experts):
        at = chip * chip_features
        for part in range(out.shape[0] // capacity):
            delta = message[
                chip * capacity : (chip + 1) * capacity,
                width + part * chip_features : width + (part + 1) * chip_features,
            ]
            rows = slice(part * capacity, (part + 1) * capacity)
            out[rows, at : at + chip_features] = (
                routed[rows, at : at + chip_features] + delta.astype(jnp.float32)
            ).astype(jnp.bfloat16)


def expert_kernel(own, other, gate_t, up_t, down, own_out, other_out, acc_own, acc_other):
    step = pl.program_id(0)
    width = gate_t.shape[1]
    dims = (((1,), (1,)), ((), ()))
    rows = jnp.concatenate([own[:, :width], other[:, :width]], axis=0)
    gate_act = lax.dot_general(rows, gate_t[...], dims, preferred_element_type=jnp.float32)
    up_act = lax.dot_general(rows, up_t[...], dims, preferred_element_type=jnp.float32)
    hidden = (gate_act / (1.0 + jnp.exp(-gate_act)) * up_act).astype(jnp.bfloat16)
    part = jnp.dot(hidden, down[...], preferred_element_type=jnp.float32)
    count = own.shape[0]

    @pl.when(step == 0)
    def _():
        acc_own[...] = part[:count]
        acc_other[...] = part[count:]

    @pl.when(step > 0)
    def _():
        acc_own[...] += part[:count]
        acc_other[...] += part[count:]

    @pl.when(step == pl.num_programs(0) - 1)
    def _():
        own_out[...] = acc_own[...]
        other_out[...] = acc_other[...].astype(jnp.bfloat16)


def expert_half(own, other, gate_t, up_t, down):
    hidden, width = gate_t.shape
    steps = 4 if hidden % 64 == 0 else 1
    block = hidden // steps
    whole = lambda array: pl.BlockSpec(array.shape, lambda i: (0, 0))
    weights = pl.BlockSpec((block, width), lambda i: (i, 0))
    result = pl.BlockSpec((own.shape[0], width), lambda i: (0, 0))
    return pl.pallas_call(
        expert_kernel,
        grid=(steps,),
        in_specs=[whole(own), whole(other), weights, weights, weights],
        out_specs=[result, result],
        out_shape=[
            jax.ShapeDtypeStruct((own.shape[0], width), jnp.float32),
            jax.ShapeDtypeStruct((own.shape[0], width), jnp.bfloat16),
        ],
        scratch_shapes=[
            pltpu.VMEM((own.shape[0], width), jnp.float32),
            pltpu.VMEM((own.shape[0], width), jnp.float32),
        ],
        name="expert_half",
    )(own, other, gate_t, up_t, down)


def to_rows(values, capacity):
    chips, tok, features = values.shape
    parts = values.reshape(chips, tok // capacity, capacity, features)
    return parts.transpose(0, 2, 1, 3).reshape(chips * capacity, tok // capacity * features)


def from_rows(rows, chips, features):
    capacity = rows.shape[0] // chips
    parts = rows.reshape(chips, capacity, rows.shape[1] // features, features)
    return parts.transpose(0, 2, 1, 3).reshape(chips, -1, features)


def per_device(
    tokens,
    routed_expert_index,
    routing_gate_weight,
    token_adapter_index,
    gate_weight_pieces,
    up_weight,
    down_weight,
    adapter_down_matrix,
    adapter_up_matrix,
):
    chips = lax.axis_size("chip")
    core = lax.axis_index("core")
    devices = chips * CORES
    experts = chips
    tok_dev, width = tokens.shape
    capacity = 2 * (tok_dev * TOP // devices + 1)
    feature_rows = adapter_down_matrix.shape[0]
    chip_features = CORES * feature_rows
    slots = experts * capacity
    extra = tok_dev // capacity * chip_features
    sizes = dict(experts=experts, capacity=capacity, chip_features=chip_features)
    aligned = capacity % 8 == 0 and chip_features % 128 == 0
    swap = lambda value: lax.ppermute(value, "core", [(0, 1), (1, 0)])

    ids_t, gates_t = routed_expert_index.T, routing_gate_weight.T
    if aligned:
        message, combine = pl.pallas_call(
            functools.partial(pack_kernel, **sizes),
            out_shape=[
                jax.ShapeDtypeStruct((slots, width + extra), jnp.bfloat16),
                jax.ShapeDtypeStruct((slots, tok_dev), jnp.float32),
            ],
            name="pack",
        )(tokens, ids_t, gates_t)
    else:
        placed, combine = slot_tables(ids_t, gates_t, experts, capacity)
        rows = jnp.dot(placed.astype(jnp.bfloat16), tokens, preferred_element_type=jnp.float32)
        columns = tokens.reshape(tok_dev, chips, chip_features).transpose(1, 0, 2)
        message = jnp.concatenate([rows.astype(jnp.bfloat16), to_rows(columns, capacity)], axis=1)

    own = lax.all_to_all(
        message.reshape(chips, capacity, width + extra), "chip", split_axis=0, concat_axis=0, tiled=True
    ).reshape(slots, width + extra)
    other = swap(own)

    by_core = token_adapter_index.reshape(chips, CORES, tok_dev)
    order = jnp.where(
        core == 0,
        jnp.stack([by_core[:, 0], by_core[:, 1]]),
        jnp.stack([by_core[:, 1], by_core[:, 0]]),
    ).reshape(-1)
    adapters = adapter_down_matrix.shape[1] // ADAPTER_RANK
    down_selected = adapter_down_matrix.reshape(feature_rows, adapters, ADAPTER_RANK)[:, order, :]
    up_selected = adapter_up_matrix.reshape(feature_rows, adapters, ADAPTER_RANK)[:, order, :]
    columns = jnp.stack(
        [from_rows(own[:, width:], chips, chip_features), from_rows(other[:, width:], chips, chip_features)]
    ).reshape(devices * tok_dev, chip_features)
    columns = jnp.where(core == 0, columns[:, :feature_rows], columns[:, feature_rows:])
    terms = jnp.einsum("tf,ftr->tr", columns, down_selected, preferred_element_type=jnp.float32)
    terms = terms.reshape(2, -1, 128)
    terms = terms + swap(terms)[::-1]
    step = 1
    while step < chips:
        terms = terms + lax.ppermute(terms, "chip", [(i, i ^ step) for i in range(chips)])
        step *= 2
    low_rank = terms.reshape(-1, ADAPTER_RANK).astype(jnp.bfloat16)
    correction = jnp.einsum("tr,ftr->tf", low_rank, up_selected, preferred_element_type=jnp.float32)
    correction = correction.astype(jnp.bfloat16).reshape(2, chips, tok_dev, feature_rows)

    own_part, other_part = expert_half(
        own, other, gate_weight_pieces[0].T, up_weight[0].T, down_weight[0]
    )
    from_sibling = swap(other_part)
    sibling_correction = swap(correction[1])
    own_correction = correction[0]
    both = jnp.where(
        core == 0,
        jnp.concatenate([own_correction, sibling_correction], axis=-1),
        jnp.concatenate([sibling_correction, own_correction], axis=-1),
    )
    summed = (own_part + from_sibling.astype(jnp.float32)).astype(jnp.bfloat16)
    reply = jnp.concatenate([summed, to_rows(both, capacity)], axis=1)
    returned = lax.all_to_all(
        reply.reshape(chips, capacity, width + extra), "chip", split_axis=0, concat_axis=0, tiled=True
    ).reshape(slots, width + extra)

    if aligned:
        return pl.pallas_call(
            functools.partial(finish_kernel, **sizes),
            out_shape=jax.ShapeDtypeStruct((tok_dev, width), jnp.bfloat16),
            name="finish",
        )(returned, combine)
    routed = weighted_rows(combine, returned[:, :width])
    delta = from_rows(returned[:, width:], chips, chip_features).transpose(1, 0, 2).reshape(tok_dev, width)
    return (routed + delta.astype(jnp.float32)).astype(jnp.bfloat16)


def solution(mesh):
    groups, devices = mesh.shape["grp"], mesh.shape["exp"]
    split = Mesh(mesh.devices.reshape(groups, devices // CORES, CORES), ("grp", "chip", "core"))
    exp = ("chip", "core")
    rows = P(("grp",) + exp, None)
    placed = (rows, rows, rows, P("grp")) + (P(exp, None, None),) * 3 + (P(exp, None),) * 2
    return jax.shard_map(per_device, mesh=split, in_specs=placed, out_specs=rows, check_vma=False)
```

```python
import functools

import jax
import jax.numpy as jnp
from jax import lax
from jax.experimental import pallas as pl
from jax.experimental.pallas import tpu as pltpu
from jax.sharding import Mesh, PartitionSpec as P

TOP = 6
ADAPTER_RANK = 16
CORES = 2


def slot_tables(ids_t, gates_t, experts, capacity):
    tok = ids_t.shape[1]
    shape = (experts * capacity, tok)
    row = lax.broadcasted_iota(jnp.int32, shape, 0)
    expert = row // capacity
    chosen = jnp.zeros(shape, jnp.float32)
    weight = jnp.zeros(shape, jnp.float32)
    for k in range(TOP):
        hit = expert == ids_t[k : k + 1, :]
        chosen = chosen + jnp.where(hit, 1.0, 0.0)
        weight = weight + jnp.where(hit, gates_t[k : k + 1, :], 0.0)
    earlier = (
        lax.broadcasted_iota(jnp.int32, (tok, tok), 0) < lax.broadcasted_iota(jnp.int32, (tok, tok), 1)
    ).astype(jnp.float32)
    position = jnp.dot(
        chosen.astype(jnp.bfloat16), earlier.astype(jnp.bfloat16), preferred_element_type=jnp.float32
    )
    slot = (row - expert * capacity).astype(jnp.float32)
    placed = jnp.where(position == slot, chosen, 0.0)
    return placed, placed * weight


def pack_kernel(tokens, ids_t, gates_t, message, combine, *, experts, capacity, chip_features):
    width = tokens.shape[1]
    placed, weighted = slot_tables(ids_t[...], gates_t[...], experts, capacity)
    combine[...] = weighted
    message[:, :width] = jnp.dot(
        placed.astype(jnp.bfloat16), tokens[...], preferred_element_type=jnp.float32
    ).astype(jnp.bfloat16)
    for chip in range(experts):
        for part in range(tokens.shape[0] // capacity):
            message[
                chip * capacity : (chip + 1) * capacity,
                width + part * chip_features : width + (part + 1) * chip_features,
            ] = tokens[
                part * capacity : (part + 1) * capacity,
                chip * chip_features : (chip + 1) * chip_features,
            ]


def weighted_rows(combine, rows):
    high = combine.astype(jnp.bfloat16)
    low = (combine - high.astype(jnp.float32)).astype(jnp.bfloat16)
    dims = (((0,), (0,)), ((), ()))
    return lax.dot_general(high, rows, dims, preferred_element_type=jnp.float32) + lax.dot_general(
        low, rows, dims, preferred_element_type=jnp.float32
    )


def finish_kernel(message, combine, out, *, experts, capacity, chip_features):
    width = out.shape[1]
    routed = weighted_rows(combine[...], message[:, :width])
    for chip in range(experts):
        at = chip * chip_features
        for part in range(out.shape[0] // capacity):
            delta = message[
                chip * capacity : (chip + 1) * capacity,
                width + part * chip_features : width + (part + 1) * chip_features,
            ]
            rows = slice(part * capacity, (part + 1) * capacity)
            out[rows, at : at + chip_features] = (
                routed[rows, at : at + chip_features] + delta.astype(jnp.float32)
            ).astype(jnp.bfloat16)


def hidden_kernel(own, other, gate_t, up_t, hidden):
    width = gate_t.shape[1]
    dims = (((1,), (1,)), ((), ()))
    rows = jnp.concatenate([own[:, :width], other[:, :width]], axis=0)
    gate_act = lax.dot_general(rows, gate_t[...], dims, preferred_element_type=jnp.float32)
    up_act = lax.dot_general(rows, up_t[...], dims, preferred_element_type=jnp.float32)
    hidden[...] = (gate_act / (1.0 + jnp.exp(-gate_act)) * up_act).astype(jnp.bfloat16)


def hidden_part(own, other, gate_t, up_t, part):
    size, width = gate_t.shape[0] // 2, gate_t.shape[1]
    count = own.shape[0] + other.shape[0]
    whole = lambda array: pl.BlockSpec(array.shape, lambda i: (0, 0))
    weights = pl.BlockSpec((size, width), lambda i: (part, 0))
    return pl.pallas_call(
        hidden_kernel,
        grid=(1,),
        in_specs=[whole(own), whole(other), weights, weights],
        out_specs=pl.BlockSpec((count, size), lambda i: (0, 0)),
        out_shape=jax.ShapeDtypeStruct((count, size), jnp.bfloat16),
        name="hidden_part",
    )(own, other, gate_t, up_t)


def down_kernel(first, second, down, out):
    size = first.shape[1]
    out[...] = (
        jnp.dot(first[...], down[:size], preferred_element_type=jnp.float32)
        + jnp.dot(second[...], down[size:], preferred_element_type=jnp.float32)
    ).astype(out.dtype)


def down_part(first, second, down, half, dtype):
    rows, size = first.shape[0] // 2, first.shape[1]
    acts = pl.BlockSpec((rows, size), lambda i: (half, 0))
    whole = pl.BlockSpec(down.shape, lambda i: (0, 0))
    return pl.pallas_call(
        down_kernel,
        grid=(1,),
        in_specs=[acts, acts, whole],
        out_specs=pl.BlockSpec((rows, down.shape[1]), lambda i: (0, 0)),
        out_shape=jax.ShapeDtypeStruct((rows, down.shape[1]), dtype),
        name="down_part",
    )(first, second, down)


def to_rows(values, capacity):
    chips, tok, features = values.shape
    parts = values.reshape(chips, tok // capacity, capacity, features)
    return parts.transpose(0, 2, 1, 3).reshape(chips * capacity, tok // capacity * features)


def from_rows(rows, chips, features):
    capacity = rows.shape[0] // chips
    parts = rows.reshape(chips, capacity, rows.shape[1] // features, features)
    return parts.transpose(0, 2, 1, 3).reshape(chips, -1, features)


def per_device(
    tokens,
    routed_expert_index,
    routing_gate_weight,
    token_adapter_index,
    gate_weight_pieces,
    up_weight,
    down_weight,
    adapter_down_matrix,
    adapter_up_matrix,
):
    chips = lax.axis_size("chip")
    core = lax.axis_index("core")
    devices = chips * CORES
    experts = chips
    tok_dev, width = tokens.shape
    capacity = 2 * (tok_dev * TOP // devices + 1)
    feature_rows = adapter_down_matrix.shape[0]
    chip_features = CORES * feature_rows
    slots = experts * capacity
    extra = tok_dev // capacity * chip_features
    sizes = dict(experts=experts, capacity=capacity, chip_features=chip_features)
    aligned = capacity % 8 == 0 and chip_features % 128 == 0
    swap = lambda value: lax.ppermute(value, "core", [(0, 1), (1, 0)])

    ids_t, gates_t = routed_expert_index.T, routing_gate_weight.T
    if aligned:
        message, combine = pl.pallas_call(
            functools.partial(pack_kernel, **sizes),
            out_shape=[
                jax.ShapeDtypeStruct((slots, width + extra), jnp.bfloat16),
                jax.ShapeDtypeStruct((slots, tok_dev), jnp.float32),
            ],
            name="pack",
        )(tokens, ids_t, gates_t)
    else:
        placed, combine = slot_tables(ids_t, gates_t, experts, capacity)
        rows = jnp.dot(placed.astype(jnp.bfloat16), tokens, preferred_element_type=jnp.float32)
        columns = tokens.reshape(tok_dev, chips, chip_features).transpose(1, 0, 2)
        message = jnp.concatenate([rows.astype(jnp.bfloat16), to_rows(columns, capacity)], axis=1)

    own = lax.all_to_all(
        message.reshape(chips, capacity, width + extra), "chip", split_axis=0, concat_axis=0, tiled=True
    )

    by_core = token_adapter_index.reshape(chips, CORES, tok_dev)
    order = jnp.where(
        core == 0,
        jnp.stack([by_core[:, 0], by_core[:, 1]]),
        jnp.stack([by_core[:, 1], by_core[:, 0]]),
    ).reshape(-1)
    adapters = adapter_down_matrix.shape[1] // ADAPTER_RANK
    held = chips * tok_dev

    def slabs(matrix):
        table = matrix.reshape(feature_rows, adapters, ADAPTER_RANK)
        chosen = table[:, order, :].transpose(1, 2, 0)
        mine, theirs = chosen[:held], swap(chosen[held:])
        return jnp.where(
            core == 0,
            jnp.concatenate([mine, theirs], axis=-1),
            jnp.concatenate([theirs, mine], axis=-1),
        )

    own, down_selected, up_selected = lax.optimization_barrier(
        (own, slabs(adapter_down_matrix), slabs(adapter_up_matrix))
    )
    own = own.reshape(slots, width + extra)
    other = swap(own)
    columns = from_rows(own[:, width:], chips, chip_features).reshape(held, chip_features)
    terms = jnp.einsum("tf,trf->tr", columns, down_selected, preferred_element_type=jnp.float32)
    terms = terms.reshape(-1, 128)

    gate_t, up_t, down = gate_weight_pieces[0].T, up_weight[0].T, down_weight[0]
    pieces = [
        lambda done: hidden_part(own, other, gate_t, up_t, 0),
        lambda done: hidden_part(own, other, gate_t, up_t, 1),
        lambda done: down_part(done[0], done[1], down, 1, jnp.bfloat16),
        lambda done: down_part(done[0], done[1], down, 0, jnp.float32),
    ]
    done = []
    step = 1
    while step < chips or len(done) < len(pieces):
        arrived = jnp.zeros_like(terms)
        if step < chips:
            arrived = lax.ppermute(terms, "chip", [(i, i ^ step) for i in range(chips)])
        if len(done) < len(pieces):
            done.append(pieces[len(done)](done))
        terms, arrived, own, other, done = lax.optimization_barrier((terms, arrived, own, other, done))
        terms = terms + arrived
        step *= 2
    other_part, own_part = done[2], done[3]
    low_rank = terms.reshape(-1, ADAPTER_RANK).astype(jnp.bfloat16)
    correction = jnp.einsum("tr,trf->tf", low_rank, up_selected, preferred_element_type=jnp.float32)
    correction = correction.astype(jnp.bfloat16).reshape(chips, tok_dev, chip_features)
    from_sibling = swap(other_part)
    summed = (own_part + from_sibling.astype(jnp.float32)).astype(jnp.bfloat16)
    reply = jnp.concatenate([summed, to_rows(correction, capacity)], axis=1)
    returned = lax.all_to_all(
        reply.reshape(chips, capacity, width + extra), "chip", split_axis=0, concat_axis=0, tiled=True
    ).reshape(slots, width + extra)

    if aligned:
        return pl.pallas_call(
            functools.partial(finish_kernel, **sizes),
            out_shape=jax.ShapeDtypeStruct((tok_dev, width), jnp.bfloat16),
            name="finish",
        )(returned, combine)
    routed = weighted_rows(combine, returned[:, :width])
    delta = from_rows(returned[:, width:], chips, chip_features).transpose(1, 0, 2).reshape(tok_dev, width)
    return (routed + delta.astype(jnp.float32)).astype(jnp.bfloat16)


def solution(mesh):
    groups, devices = mesh.shape["grp"], mesh.shape["exp"]
    split = Mesh(mesh.devices.reshape(groups, devices // CORES, CORES), ("grp", "chip", "core"))
    exp = ("chip", "core")
    rows = P(("grp",) + exp, None)
    placed = (rows, rows, rows, P("grp")) + (P(exp, None, None),) * 3 + (P(exp, None),) * 2
    return jax.shard_map(per_device, mesh=split, in_specs=placed, out_specs=rows, check_vma=False)
```

```python
import functools

import jax
import jax.numpy as jnp
from jax import lax
from jax.experimental import pallas as pl
from jax.experimental.pallas import tpu as pltpu
from jax.sharding import Mesh, PartitionSpec as P

TOP = 6
ADAPTER_RANK = 16
CORES = 2


def slot_tables(ids_t, gates_t, experts, capacity):
    tok = ids_t.shape[1]
    shape = (experts * capacity, tok)
    row = lax.broadcasted_iota(jnp.int32, shape, 0)
    expert = row // capacity
    chosen = jnp.zeros(shape, jnp.float32)
    weight = jnp.zeros(shape, jnp.float32)
    for k in range(TOP):
        hit = expert == ids_t[k : k + 1, :]
        chosen = chosen + jnp.where(hit, 1.0, 0.0)
        weight = weight + jnp.where(hit, gates_t[k : k + 1, :], 0.0)
    earlier = (
        lax.broadcasted_iota(jnp.int32, (tok, tok), 0) < lax.broadcasted_iota(jnp.int32, (tok, tok), 1)
    ).astype(jnp.float32)
    position = jnp.dot(
        chosen.astype(jnp.bfloat16), earlier.astype(jnp.bfloat16), preferred_element_type=jnp.float32
    )
    slot = (row - expert * capacity).astype(jnp.float32)
    placed = jnp.where(position == slot, chosen, 0.0)
    return placed, placed * weight


def pack_kernel(tokens, ids_t, gates_t, message, combine, *, experts, capacity, chip_features):
    width = tokens.shape[1]
    placed, weighted = slot_tables(ids_t[...], gates_t[...], experts, capacity)
    combine[...] = weighted
    message[:, :width] = jnp.dot(
        placed.astype(jnp.bfloat16), tokens[...], preferred_element_type=jnp.float32
    ).astype(jnp.bfloat16)
    for chip in range(experts):
        for part in range(tokens.shape[0] // capacity):
            message[
                chip * capacity : (chip + 1) * capacity,
                width + part * chip_features : width + (part + 1) * chip_features,
            ] = tokens[
                part * capacity : (part + 1) * capacity,
                chip * chip_features : (chip + 1) * chip_features,
            ]


def weighted_rows(combine, rows):
    high = combine.astype(jnp.bfloat16)
    low = (combine - high.astype(jnp.float32)).astype(jnp.bfloat16)
    dims = (((0,), (0,)), ((), ()))
    return lax.dot_general(high, rows, dims, preferred_element_type=jnp.float32) + lax.dot_general(
        low, rows, dims, preferred_element_type=jnp.float32
    )


def finish_kernel(message, combine, out, *, experts, capacity, chip_features):
    width = out.shape[1]
    routed = weighted_rows(combine[...], message[:, :width])
    for chip in range(experts):
        at = chip * chip_features
        for part in range(out.shape[0] // capacity):
            delta = message[
                chip * capacity : (chip + 1) * capacity,
                width + part * chip_features : width + (part + 1) * chip_features,
            ]
            rows = slice(part * capacity, (part + 1) * capacity)
            out[rows, at : at + chip_features] = (
                routed[rows, at : at + chip_features] + delta.astype(jnp.float32)
            ).astype(jnp.bfloat16)


def column_steps(width):
    return width // 512 if width % 512 == 0 else 1


def hidden_kernel(own, other, gate_t, up_t, hidden, gate_act, up_act):
    step = pl.program_id(0)
    dims = (((1,), (1,)), ((), ()))
    rows = jnp.concatenate([own[...], other[...]], axis=0)
    gate_part = lax.dot_general(rows, gate_t[...], dims, preferred_element_type=jnp.float32)
    up_part = lax.dot_general(rows, up_t[...], dims, preferred_element_type=jnp.float32)

    @pl.when(step == 0)
    def _():
        gate_act[...] = gate_part
        up_act[...] = up_part

    @pl.when(step > 0)
    def _():
        gate_act[...] += gate_part
        up_act[...] += up_part

    @pl.when(step == pl.num_programs(0) - 1)
    def _():
        act = gate_act[...]
        hidden[...] = (act / (1.0 + jnp.exp(-act)) * up_act[...]).astype(jnp.bfloat16)


def hidden_part(own, other, gate_t, up_t):
    size, width = gate_t.shape
    steps = column_steps(width)
    count = own.shape[0] + other.shape[0]
    cut = lambda array: pl.BlockSpec((array.shape[0], width // steps), lambda i: (0, i))
    return pl.pallas_call(
        hidden_kernel,
        grid=(steps,),
        in_specs=[cut(own), cut(other), cut(gate_t), cut(up_t)],
        out_specs=pl.BlockSpec((count, size), lambda i: (0, 0)),
        out_shape=jax.ShapeDtypeStruct((count, size), jnp.bfloat16),
        scratch_shapes=[pltpu.VMEM((count, size), jnp.float32)] * 2,
        name="hidden_part",
    )(own, other, gate_t, up_t)


def down_kernel(hidden, down, own_out, other_out):
    out = jnp.dot(hidden[...], down[...], preferred_element_type=jnp.float32)
    own_out[...] = out[: own_out.shape[0]]
    other_out[...] = out[own_out.shape[0] :].astype(jnp.bfloat16)


def down_part(hidden, down):
    rows, width = hidden.shape[0] // 2, down.shape[1]
    steps = column_steps(width)
    cut = lambda count: pl.BlockSpec((count, width // steps), lambda i: (0, i))
    return pl.pallas_call(
        down_kernel,
        grid=(steps,),
        in_specs=[pl.BlockSpec(hidden.shape, lambda i: (0, 0)), cut(down.shape[0])],
        out_specs=[cut(rows), cut(rows)],
        out_shape=[
            jax.ShapeDtypeStruct((rows, width), jnp.float32),
            jax.ShapeDtypeStruct((rows, width), jnp.bfloat16),
        ],
        name="down_part",
    )(hidden, down)


def to_rows(values, capacity):
    chips, tok, features = values.shape
    parts = values.reshape(chips, tok // capacity, capacity, features)
    return parts.transpose(0, 2, 1, 3).reshape(chips * capacity, tok // capacity * features)


def from_rows(rows, chips, features):
    capacity = rows.shape[0] // chips
    parts = rows.reshape(chips, capacity, rows.shape[1] // features, features)
    return parts.transpose(0, 2, 1, 3).reshape(chips, -1, features)


def per_device(
    tokens,
    routed_expert_index,
    routing_gate_weight,
    token_adapter_index,
    gate_weight_pieces,
    up_weight,
    down_weight,
    adapter_down_matrix,
    adapter_up_matrix,
):
    chips = lax.axis_size("chip")
    core = lax.axis_index("core")
    devices = chips * CORES
    experts = chips
    tok_dev, width = tokens.shape
    capacity = 2 * (tok_dev * TOP // devices + 1)
    feature_rows = adapter_down_matrix.shape[0]
    chip_features = CORES * feature_rows
    slots = experts * capacity
    extra = tok_dev // capacity * chip_features
    sizes = dict(experts=experts, capacity=capacity, chip_features=chip_features)
    aligned = capacity % 8 == 0 and chip_features % 128 == 0
    swap = lambda value: lax.ppermute(value, "core", [(0, 1), (1, 0)])

    ids_t, gates_t = routed_expert_index.T, routing_gate_weight.T
    if aligned:
        message, combine = pl.pallas_call(
            functools.partial(pack_kernel, **sizes),
            out_shape=[
                jax.ShapeDtypeStruct((slots, width + extra), jnp.bfloat16),
                jax.ShapeDtypeStruct((slots, tok_dev), jnp.float32),
            ],
            name="pack",
        )(tokens, ids_t, gates_t)
    else:
        placed, combine = slot_tables(ids_t, gates_t, experts, capacity)
        rows = jnp.dot(placed.astype(jnp.bfloat16), tokens, preferred_element_type=jnp.float32)
        columns = tokens.reshape(tok_dev, chips, chip_features).transpose(1, 0, 2)
        message = jnp.concatenate([rows.astype(jnp.bfloat16), to_rows(columns, capacity)], axis=1)

    own = lax.all_to_all(
        message.reshape(chips, capacity, width + extra), "chip", split_axis=0, concat_axis=0, tiled=True
    )

    by_core = token_adapter_index.reshape(chips, CORES, tok_dev)
    order = jnp.where(core == 0, by_core[:, 0], by_core[:, 1]).reshape(-1)
    adapters = adapter_down_matrix.shape[1] // ADAPTER_RANK
    held = chips * tok_dev

    def slabs(matrix):
        both = jnp.concatenate([matrix, swap(matrix)], axis=0)
        table = both.reshape(chip_features, adapters, ADAPTER_RANK)
        return table[:, order, :].transpose(1, 2, 0)

    def flip(values):
        halves = values[..., feature_rows:], values[..., :feature_rows]
        return jnp.where(core == 0, values, jnp.concatenate(halves, axis=-1))

    own, down_selected, up_selected = lax.optimization_barrier(
        (own, slabs(adapter_down_matrix), slabs(adapter_up_matrix))
    )
    own = own.reshape(slots, width + extra)
    other = swap(own)
    columns = from_rows(own[:, width:], chips, chip_features).reshape(held, chip_features)
    terms = jnp.einsum("tf,trf->tr", flip(columns), down_selected, preferred_element_type=jnp.float32)
    terms = terms.reshape(-1, 128)

    gate_t, up_t, down = gate_weight_pieces[0].T, up_weight[0].T, down_weight[0]
    pieces = [
        lambda done: hidden_part(own, other, gate_t, up_t),
        lambda done: down_part(done[0], down),
    ]
    done = []
    step = 1
    while step < chips or len(done) < len(pieces):
        arrived = jnp.zeros_like(terms)
        if step < chips:
            arrived = lax.ppermute(terms, "chip", [(i, i ^ step) for i in range(chips)])
        if len(done) < len(pieces):
            done.append(pieces[len(done)](done))
        terms, arrived, own, other, done = lax.optimization_barrier((terms, arrived, own, other, done))
        terms = terms + arrived
        step *= 2
    own_part, other_part = done[1]
    low_rank = terms.reshape(-1, ADAPTER_RANK).astype(jnp.bfloat16)
    correction = jnp.einsum("tr,trf->tf", low_rank, up_selected, preferred_element_type=jnp.float32)
    correction = flip(correction.astype(jnp.bfloat16)).reshape(chips, tok_dev, chip_features)
    from_sibling = swap(other_part)
    summed = (own_part + from_sibling.astype(jnp.float32)).astype(jnp.bfloat16)
    reply = jnp.concatenate([summed, to_rows(correction, capacity)], axis=1)
    returned = lax.all_to_all(
        reply.reshape(chips, capacity, width + extra), "chip", split_axis=0, concat_axis=0, tiled=True
    ).reshape(slots, width + extra)

    if aligned:
        return pl.pallas_call(
            functools.partial(finish_kernel, **sizes),
            out_shape=jax.ShapeDtypeStruct((tok_dev, width), jnp.bfloat16),
            name="finish",
        )(returned, combine)
    routed = weighted_rows(combine, returned[:, :width])
    delta = from_rows(returned[:, width:], chips, chip_features).transpose(1, 0, 2).reshape(tok_dev, width)
    return (routed + delta.astype(jnp.float32)).astype(jnp.bfloat16)


def solution(mesh):
    groups, devices = mesh.shape["grp"], mesh.shape["exp"]
    split = Mesh(mesh.devices.reshape(groups, devices // CORES, CORES), ("grp", "chip", "core"))
    exp = ("chip", "core")
    rows = P(("grp",) + exp, None)
    placed = (rows, rows, rows, P("grp")) + (P(exp, None, None),) * 3 + (P(exp, None),) * 2
    return jax.shard_map(per_device, mesh=split, in_specs=placed, out_specs=rows, check_vma=False)
```
